256 devices in a mesh: row: 8 (over y, x_lo), col: 32 (over z, x_hi, core).
Axes of the slice: x: 4 (x_hi: 2, x_lo: 2; x = x_hi * 2 + x_lo), y: 4, z: 8, core: 2. Of those that a mesh axis runs over, the one named last changes fastest.
Arguments:
- density: bfloat16 [8192, 8192], P('row', 'col'), may hold values from -0.0625 to 0.0625
- density_mask: int32 [64, 64], P('row', 'col'), may hold values from 0 to 1, as said below
- response: bfloat16 [2, 8192, 8192], P(None, 'row', 'col'), may hold values from -6 to 6
- response_mask: int32 [2, 64, 64], P(None, 'row', 'col'), may hold values from 0 to 1, as said below
- filter_mask: int32 [64, 64], P('row', 'col'), may hold values from 0 to 1, as said below
Outputs:
- product: bfloat16 [2, 8192, 8192], P(None, 'row', 'col')
The draws below stay inside these ranges and needn't reach their ends.
Inputs may be any that keep to these rules, and one draw needn't show every extreme that they name: `density_mask`: diagonal blocks are always nonzero; blocks within cyclic block distance 8 of the diagonal are more often nonzero than blocks further out; whole block rows and whole block columns may be nonzero. `response_mask`: for each direction, diagonal blocks are always nonzero; blocks within cyclic block distance 8 of the diagonal are more often nonzero than blocks further out; whole block rows and whole block columns may be nonzero. `filter_mask`: diagonal blocks are always kept; blocks within cyclic block distance 2 * 8 of the diagonal are more often kept than blocks further out; whole block rows and whole block columns may be kept.
All inputs are finite; a program needn't handle non-finite values.
Results may differ from the reference program's by a relative error of at most 0.001.
Values may be sent and summed in bfloat16 or wider, within the bound.
No kernel may reach another device: no remote copies, remote signals or barrier semaphores. Data moves between devices by JAX's collectives and lax.ppermute only.
A program may use at most 128 MiB of HBM per device.

```python
import jax
import jax.numpy as jnp

BLOCK = 128
NB_UNIT = 2
NB = 64
SLAB_ROWS = 8
BAND = 8
N = 8192


def banded_pattern(key, keep_near, keep_far, reach):
    first = jnp.arange(NB, dtype=jnp.int32)[:, None]
    second = jnp.arange(NB, dtype=jnp.int32)[None, :]
    spacing = jnp.abs(first - second)
    distance = jnp.minimum(spacing, NB - spacing)
    rolled = jax.random.randint(jax.random.fold_in(key, 1), (NB, NB), 0, 100, dtype=jnp.int32)
    kept = jnp.where(distance <= reach, rolled < keep_near, rolled < keep_far)
    kept = jnp.logical_or(kept, distance == 0)
    row_group = jax.random.randint(jax.random.fold_in(key, 2), (), 0, NB // SLAB_ROWS, dtype=jnp.int32)
    col_group = jax.random.randint(jax.random.fold_in(key, 3), (), 0, NB // NB_UNIT, dtype=jnp.int32)
    full_rows = first // SLAB_ROWS == row_group
    full_cols = second // NB_UNIT == col_group
    kept = jnp.logical_or(kept, jnp.logical_or(full_rows, full_cols))
    return kept.astype(jnp.int32)


def draw_density_mask(key, part):
    return banded_pattern(jax.random.fold_in(key, 11), 80, 8, BAND)


def draw_response_mask(key, part):
    first = banded_pattern(jax.random.fold_in(key, 21), 80, 8, BAND)
    second = banded_pattern(jax.random.fold_in(key, 22), 80, 8, BAND)
    return jnp.stack([first, second])


def draw_filter_mask(key, part):
    return banded_pattern(jax.random.fold_in(key, 31), 90, 25, 2 * BAND)


def block_levels(key, shape, shards, low, high):
    def one(position, blocks):
        draws = jax.random.uniform(jax.random.fold_in(jax.random.fold_in(key, 6), position), (blocks,), jnp.float32, low / len(shards), high / len(shards))
        return jnp.repeat(jnp.exp(draws), shape[position] // blocks).reshape((-1,) + (1,) * (len(shape) - position - 1))

    factor_of = one(*shards[0])
    for cut in shards[1:]:
        factor_of = factor_of * one(*cut)
    return factor_of


def noise(rng, shape, spread, most, pieces=(), kind=jnp.bfloat16):
    drawn = jax.random.normal(rng, shape, jnp.float32) * spread
    if len(pieces) > 0:
        drawn = block_levels(rng, shape, pieces, -0.22, 0.18) * drawn
    return jnp.clip(drawn, min=-most, max=most).astype(kind)


def setup_inputs(seed: int = 0) -> dict:
    key_of = jax.random.split(jax.random.key(seed), 6)
    density = noise(key_of[0], (N, N), N ** -0.5, 0.0625, ((0, 8), (1, 32)))
    density_mask = draw_density_mask(jax.random.fold_in(key_of[5], 71), 0)
    response = noise(key_of[2], (2, N, N), 1.0, 6.0, ((1, 8), (2, 32)))
    response_mask = draw_response_mask(jax.random.fold_in(key_of[5], 71), 0)
    filter_mask = draw_filter_mask(jax.random.fold_in(key_of[5], 71), 0)
    return dict(density=density, density_mask=density_mask, response=response, response_mask=response_mask, filter_mask=filter_mask)


def expand_blocks(values, mask, blocksize):
    lead = values.shape[:-2]
    height = values.shape[-2] // blocksize
    width = values.shape[-1] // blocksize
    shaped = values.reshape(lead + (height, blocksize, width, blocksize))
    scaled = shaped * mask.astype(values.dtype)[..., :, None, :, None]
    return scaled.reshape(values.shape)


def reference(density, density_mask, response, response_mask, filter_mask):
    masked_density = expand_blocks(density, density_mask, BLOCK)
    masked_response = expand_blocks(response, response_mask, BLOCK)
    first = jnp.dot(masked_density, masked_response[0], preferred_element_type=jnp.float32)
    second = jnp.dot(masked_density, masked_response[1], preferred_element_type=jnp.float32)
    stacked = jnp.stack([first, second])
    return expand_blocks(stacked, filter_mask, BLOCK).astype(jnp.bfloat16)
```

```python
import functools

import jax
import jax.numpy as jnp
from jax import lax
from jax.experimental import pallas as pl
from jax.experimental.pallas import tpu as pltpu
from jax.sharding import PartitionSpec as P


BLOCK = 128
ROWS = 1024
COLS = 256
NZ, NY = 8, 4


def col_moves(step):
    pairs = []
    for c in range(32):
        z, hi, core = step(c // 4, (c // 2) % 2, c % 2)
        pairs.append((c, (z % NZ) * 4 + (hi % 2) * 2 + core % 2))
    return pairs


def along_z(v):
    pairs = col_moves(lambda z, hi, core: (z + 1 - 2 * core, hi, core))
    return lax.ppermute(v, "col", pairs)


def across_x(v):
    return lax.ppermute(v, "col", col_moves(lambda z, hi, core: (z, hi + 1, core)))


def other_core(v):
    return lax.ppermute(v, "col", col_moves(lambda z, hi, core: (z, hi, core + 1)))


def along_y(v):
    pairs = []
    for r in range(8):
        for c in range(32):
            y = (r // 2 + 1 - 2 * (c % 2)) % NY
            pairs.append((r * 32 + c, (y * 2 + r % 2) * 32 + c))
    return lax.ppermute(v, ("row", "col"), pairs)


def beside_x(v):
    return lax.ppermute(v, "row", [(r, r ^ 1) for r in range(8)])


def expand_blocks(values, mask):
    lead = values.shape[:-2]
    height = values.shape[-2] // BLOCK
    width = values.shape[-1] // BLOCK
    shaped = values.reshape(lead + (height, BLOCK, width, BLOCK))
    scaled = shaped * mask.astype(values.dtype)[..., :, None, :, None]
    return scaled.reshape(values.shape)


def matmul_kernel(n_a, n_b, table, keep, *refs):
    a_refs, b_refs = refs[:n_a], refs[n_a : n_a + n_b]
    out, a_vm, b_vm, acc, a_sem, b_sem = refs[n_a + n_b :]
    b_copies = []
    for i, ref in enumerate(b_refs):
        at = pl.ds(pl.multiple_of(table[2, i] * ROWS, ROWS), ROWS)
        b_copies.append(pltpu.make_async_copy(ref, b_vm.at[:, at, :], b_sem.at[i]))
        b_copies[-1].start()
    a_copies = []
    for i, ref in enumerate(a_refs):
        pair = []
        for j in range(2):
            at = pl.ds(pl.multiple_of(table[j, i] * COLS, COLS), COLS)
            pair.append(pltpu.make_async_copy(ref.at[j], a_vm.at[:, at], a_sem.at[2 * i + j]))
            pair[-1].start()
        a_copies.append(pair)
    for copy in b_copies:
        copy.wait()
    for step in range(8):
        for pair in a_copies[2 * step : 2 * step + 2]:
            for copy in pair:
                copy.wait()
        start = pl.multiple_of(table[3, step] * ROWS, ROWS)

        def rows(t, _):
            at = pl.ds(pl.multiple_of(t * 256, 256), 256)
            left = a_vm[at, pl.ds(start, ROWS)]
            for d in range(2):
                part = jnp.dot(
                    left, b_vm[d, pl.ds(start, ROWS), :], preferred_element_type=jnp.float32
                )
                if step == 0:
                    acc[d, at, :] = part
                elif step < 7:
                    acc[d, at, :] += part
                else:
                    total = acc[d, at, :] + part
                    for i in range(2):
                        for j in range(2):
                            scale = keep[t * 2 + i, j].astype(jnp.float32)
                            block = total[i * BLOCK : (i + 1) * BLOCK, j * BLOCK : (j + 1) * BLOCK]
                            out[
                                d,
                                pl.ds(pl.multiple_of(t * 256 + i * BLOCK, BLOCK), BLOCK),
                                j * BLOCK : (j + 1) * BLOCK,
                            ] = (block * scale).astype(jnp.bfloat16)
            return 0

        lax.fori_loop(0, 4, rows, 0)


def multiply(table, keep, a_parts, b_parts):
    n_a, n_b = len(a_parts), len(b_parts)
    anywhere = pl.BlockSpec(memory_space=pl.ANY)
    scalars = pl.BlockSpec(memory_space=pltpu.SMEM)
    return pl.pallas_call(
        functools.partial(matmul_kernel, n_a, n_b),
        out_shape=jax.ShapeDtypeStruct((2, ROWS, COLS), jnp.bfloat16),
        in_specs=[scalars, scalars] + [anywhere] * (n_a + n_b),
        out_specs=pl.BlockSpec(memory_space=pltpu.VMEM),
        scratch_shapes=[
            pltpu.VMEM((ROWS, 8 * ROWS), jnp.bfloat16),
            pltpu.VMEM((2, 8 * ROWS, COLS), jnp.bfloat16),
            pltpu.VMEM((2, ROWS, COLS), jnp.float32),
            pltpu.SemaphoreType.DMA((2 * n_a,)),
            pltpu.SemaphoreType.DMA((n_b,)),
        ],
        compiler_params=pltpu.CompilerParams(vmem_limit_bytes=40 * 2**20),
        cost_estimate=pl.CostEstimate(
            flops=2 * 2 * ROWS * COLS * 8 * ROWS, bytes_accessed=25 * 2**20, transcendentals=0
        ),
    )(table, keep, *a_parts, *b_parts)


def body(density, density_mask, response, response_mask, filter_mask):
    own = expand_blocks(density, density_mask)
    b0 = expand_blocks(response, response_mask)

    row, col = lax.axis_index("row"), lax.axis_index("col")
    y, lo = row // 2, row % 2
    z, hi, core = col // 4, (col // 2) % 2, col % 2
    way = 1 - 2 * core

    side = beside_x(b0)
    across = across_x(own)
    p0 = jnp.stack([own, other_core(own)])
    p1 = along_z(p0)
    r1 = along_y(b0)
    q0 = jnp.stack([across, other_core(across)])
    p1o = other_core(p1)
    p2 = along_z(p1)
    r2 = along_y(r1)
    p2o = other_core(p2)
    p3 = along_z(p2)
    r3 = along_y(r2)
    q1 = along_z(q0)
    s1 = along_y(side)
    q3 = across_x(p3)
    p3o = other_core(p3)
    q1o = other_core(q1)
    q2 = along_z(q1)
    s2 = along_y(s1)
    q2o = other_core(q2)
    q3o = other_core(q3)
    last = along_z(jnp.stack([p3[0], q3[0]]))
    s3 = along_y(s2)
    lasto = other_core(last)

    def pieces(distance, side_hi, first):
        k = ((z + distance) % NZ) * 4 + side_hi * 2
        return k + first, k + 1 - first

    near, far = hi, 1 - hi
    mine, theirs = core, 1 - core
    a_list = [
        (p0, pieces(0, near, mine)),
        (q0, pieces(0, far, mine)),
        (p1, pieces(-way, near, mine)),
        (q1, pieces(-way, far, mine)),
        (p1o, pieces(way, near, theirs)),
        (q1o, pieces(way, far, theirs)),
        (p2, pieces(-2 * way, near, mine)),
        (q2, pieces(-2 * way, far, mine)),
        (p2o, pieces(2 * way, near, theirs)),
        (q2o, pieces(2 * way, far, theirs)),
        (p3, pieces(-3 * way, near, mine)),
        (q3, pieces(-3 * way, far, mine)),
        (p3o, pieces(3 * way, near, theirs)),
        (q3o, pieces(3 * way, far, theirs)),
    ]
    k4 = ((z + 4) % NZ) * 4
    a_list += [
        (last, (k4 + near * 2 + mine, k4 + far * 2 + mine)),
        (lasto, (k4 + near * 2 + theirs, k4 + far * 2 + theirs)),
    ]
    b_list = [(v, ((y - i * way) % NY) * 2 + lo) for i, v in enumerate([b0, r1, r2, r3])]
    b_list += [(v, ((y - i * way) % NY) * 2 + 1 - lo) for i, v in enumerate([side, s1, s2, s3])]
    order = [(z + s * way) % NZ for s in (0, -1, 1, -2, 2, -3, 3, 4)]
    pad = [jnp.int32(0)] * 8
    table = jnp.stack(
        [
            jnp.stack([at[0] for _, at in a_list]),
            jnp.stack([at[1] for _, at in a_list]),
            jnp.stack([at for _, at in b_list] + pad),
            jnp.stack(order + pad),
        ]
    ).astype(jnp.int32)
    return multiply(table, filter_mask, [v for v, _ in a_list], [v for v, _ in b_list])


def solution(mesh):
    in_specs = (
        P("row", "col"),
        P("row", "col"),
        P(None, "row", "col"),
        P(None, "row", "col"),
        P("row", "col"),
    )
    out_specs = P(None, "row", "col")
    return jax.shard_map(body, mesh=mesh, in_specs=in_specs, out_specs=out_specs, check_vma=False)
```

```python
import functools

import jax
import jax.numpy as jnp
from jax import lax
from jax.experimental import pallas as pl
from jax.experimental.pallas import tpu as pltpu
from jax.sharding import PartitionSpec as P


BLOCK = 128
ROWS = 1024
COLS = 256
UNIT = 512
VMEM_LIMIT = 60 * 2**20
AHEAD = 3
NZ, NY = 8, 4


def col_pairs(step):
    pairs = []
    for c in range(32):
        z, hi, core = step(c // 4, (c // 2) % 2, c % 2)
        pairs.append((c, (z % NZ) * 4 + (hi % 2) * 2 + core % 2))
    return pairs


def along_z(v):
    return lax.ppermute(v, "col", col_pairs(lambda z, hi, core: (z + 1 - 2 * core, hi, core)))


def across_x(v):
    return lax.ppermute(v, "col", col_pairs(lambda z, hi, core: (z, hi + 1, core)))


def other_core(v):
    return lax.ppermute(v, "col", col_pairs(lambda z, hi, core: (z, hi, core + 1)))


def along_y(v):
    pairs = []
    for r in range(8):
        for c in range(32):
            y = (r // 2 + 1 - 2 * (c % 2)) % NY
            pairs.append((r * 32 + c, (y * 2 + r % 2) * 32 + c))
    return lax.ppermute(v, ("row", "col"), pairs)


def beside_x(v):
    return lax.ppermute(v, "row", [(r, r ^ 1) for r in range(8)])


def mask_kernel(mask, values, out, *apart):
    for i in range(8):
        for j in range(2):
            at = (slice(i * BLOCK, (i + 1) * BLOCK), slice(j * BLOCK, (j + 1) * BLOCK))
            if not apart:
                out[at] = values[at] * mask[j, i].astype(jnp.bfloat16)
            for d, copy in enumerate(apart):
                block = values[(d, *at)] * mask[d, j, i].astype(jnp.bfloat16)
                out[(d, *at)] = block
                copy[at] = block


def masked(values, mask):
    out = [jax.ShapeDtypeStruct(values.shape, values.dtype)]
    if len(values.shape) == 3:
        out += [jax.ShapeDtypeStruct(values.shape[1:], values.dtype)] * values.shape[0]
    return pl.pallas_call(
        mask_kernel,
        out_shape=out,
        in_specs=[
            pl.BlockSpec(memory_space=pltpu.SMEM),
            pl.BlockSpec(memory_space=pltpu.VMEM),
        ],
        out_specs=[pl.BlockSpec(memory_space=pltpu.VMEM)] * len(out),
        cost_estimate=pl.CostEstimate(flops=10**6, bytes_accessed=2**20, transcendentals=0),
    )(jnp.swapaxes(mask, -1, -2), values)


def matmul_kernel(n_a, parts, n_b, pieces, place, keep, *refs):
    a_refs, refs = refs[:n_a], refs[n_a:]
    b_refs, refs = refs[:n_b], refs[n_b:]
    out, a_vm, b_vm, acc, a_sem, b_sem = refs
    row, col = place[0], place[1]
    y, lo = row // 2, row % 2
    z, hi, core = col // 4, (col // 2) % 2, col % 2
    way = 1 - 2 * core
    n_units = len(parts)

    def start(u):
        delta, far = u // 2, u % 2
        head = 1 - core if 1 <= delta <= 3 else core
        for j, (which, index) in enumerate(parts[u]):
            ref = a_refs[which] if index is None else a_refs[which].at[index]
            to = a_vm.at[u, (head + j) % 2]
            pltpu.make_async_copy(ref, to, a_sem.at[u]).start()
        owner = (z + delta * way + NZ) % NZ
        hops = ((y - owner // 2) * way + NY) % NY
        side = (owner % 2 + lo) % 2
        rows = pl.ds(pl.multiple_of(((hi + far) % 2) * UNIT, UNIT), UNIT)
        for i in range(4):
            for low in range(2):

                @pl.when(jnp.logical_and(hops == i, side == low))
                def _():
                    for which, d, at, where in pieces:
                        if (at, where) == (i, low):
                            if d is None:
                                source, target = b_refs[which].at[:, rows, :], b_vm.at[u]
                            else:
                                source, target = b_refs[which].at[rows, :], b_vm.at[u, d]
                            pltpu.make_async_copy(source, target, b_sem.at[u]).start()

    def wait(u):
        pltpu.make_async_copy(b_vm.at[u], b_vm.at[u], b_sem.at[u]).wait()
        pltpu.make_async_copy(a_vm.at[u], a_vm.at[u], a_sem.at[u]).wait()

    for u in range(AHEAD):
        start(u)
    for u in range(n_units):
        if u + AHEAD < n_units:
            start(u + AHEAD)
        wait(u)
        for d in range(2):
            part = sum(
                jnp.dot(
                    a_vm[u, c],
                    b_vm[u, d, c * COLS : (c + 1) * COLS, :],
                    preferred_element_type=jnp.float32,
                )
                for c in range(2)
            )
            if u == 0:
                acc[d] = part
            elif u < n_units - 1:
                acc[d] += part
            else:
                total = acc[d] + part
                for i in range(8):
                    for j in range(2):
                        scale = keep[j, i].astype(jnp.float32)
                        at = (slice(i * BLOCK, (i + 1) * BLOCK), slice(j * BLOCK, (j + 1) * BLOCK))
                        out[(d, *at)] = (total[at] * scale).astype(jnp.bfloat16)


def listed(arrays, array):
    for n, other in enumerate(arrays):
        if other is array:
            return n
    arrays.append(array)
    return len(arrays) - 1


def multiply(place, keep, units, b_parts):
    a_arrays, b_arrays = [], []
    parts = [[(listed(a_arrays, v), index) for v, index in unit] for unit in units]
    pieces = [(listed(b_arrays, v), d, hops, low) for v, d, hops, low in b_parts]
    n_a, n_b = len(a_arrays), len(b_arrays)
    anywhere = pl.BlockSpec(memory_space=pl.ANY)
    scalars = pl.BlockSpec(memory_space=pltpu.SMEM)
    return pl.pallas_call(
        functools.partial(matmul_kernel, n_a, parts, n_b, pieces),
        out_shape=jax.ShapeDtypeStruct((2, ROWS, COLS), jnp.bfloat16),
        in_specs=[scalars, scalars] + [anywhere] * (n_a + n_b),
        out_specs=pl.BlockSpec(memory_space=pltpu.VMEM),
        scratch_shapes=[
            pltpu.VMEM((16, 2, ROWS, COLS), jnp.bfloat16),
            pltpu.VMEM((16, 2, UNIT, COLS), jnp.bfloat16),
            pltpu.VMEM((2, ROWS, COLS), jnp.float32),
            pltpu.SemaphoreType.DMA((16,)),
            pltpu.SemaphoreType.DMA((16,)),
        ],
        compiler_params=pltpu.CompilerParams(vmem_limit_bytes=VMEM_LIMIT),
        cost_estimate=pl.CostEstimate(
            flops=2 * 2 * ROWS * COLS * 8 * ROWS, bytes_accessed=25 * 2**20, transcendentals=0
        ),
    )(place, keep, *a_arrays, *b_arrays)


def work(density, density_mask, response, response_mask, filter_mask):
    place = jnp.stack([lax.axis_index("row"), lax.axis_index("col")]).astype(jnp.int32)
    (own,) = masked(density, density_mask)
    b0, b0a, b0b = masked(response, response_mask)

    p0o, across = other_core(own), across_x(own)
    q0 = jnp.stack([across, other_core(across)])
    p1a, p1b = along_z(own), along_z(p0o)
    p2a, p2b = along_z(p1a), along_z(p1b)
    p3a, p3b = along_z(p2a), along_z(p2b)
    p1ao, p1bo = other_core(p1a), other_core(p1b)
    p2ao, p2bo = other_core(p2a), other_core(p2b)
    p3ao, p3bo = other_core(p3a), other_core(p3b)
    p4 = along_z(p3a)
    p4o = other_core(p4)
    q3a, q3b = across_x(p3a), across_x(p3b)
    q3ao, q3bo = other_core(q3a), other_core(q3b)
    q1 = along_z(q0)
    q2 = along_z(q1)
    q1o, q2o = other_core(q1), other_core(q2)
    q4 = along_z(q3a)
    q4o = other_core(q4)

    r1 = along_y(b0)
    r2 = along_y(r1)
    r3 = along_y(r2)
    s0a, s0b = beside_x(b0a), beside_x(b0b)
    s1a, s1b = along_y(s0a), along_y(s0b)
    s2a, s2b = along_y(s1a), along_y(s1b)
    s3a, s3b = along_y(s2a), along_y(s2b)

    both = lambda v: [(v, 0), (v, 1)]
    two = lambda v, w: [(v, None), (w, None)]
    units = [
        two(own, p0o), both(q0),
        two(p1ao, p1bo), both(q1o),
        two(p2ao, p2bo), both(q2o),
        two(p3ao, p3bo), two(q3ao, q3bo),
        two(p4, p4o), two(q4, q4o),
        two(p3a, p3b), two(q3a, q3b),
        two(p2a, p2b), both(q2),
        two(p1a, p1b), both(q1),
    ]
    b_parts = [(v, None, i, 0) for i, v in enumerate([b0, r1, r2, r3])]
    for i, pair in enumerate([(s0a, s0b), (s1a, s1b), (s2a, s2b), (s3a, s3b)]):
        b_parts += [(v, d, i, 1) for d, v in enumerate(pair)]
    return multiply(place, jnp.swapaxes(filter_mask, 0, 1), units, b_parts)


def solution(mesh):
    in_specs = (
        P("row", "col"),
        P("row", "col"),
        P(None, "row", "col"),
        P(None, "row", "col"),
        P("row", "col"),
    )
    out_specs = P(None, "row", "col")
    return jax.shard_map(work, mesh=mesh, in_specs=in_specs, out_specs=out_specs, check_vma=False)
```

```python
import functools

import jax
import jax.numpy as jnp
from jax import lax
from jax.experimental import pallas as pl
from jax.experimental.pallas import tpu as pltpu
from jax.sharding import PartitionSpec as P


BLOCK = 128
ROWS = 1024
COLS = 256
UNIT = 512
VMEM_LIMIT = 60 * 2**20
AHEAD = 3
NZ, NY = 8, 4


def col_pairs(step):
    pairs = []
    for c in range(32):
        z, hi, core = step(c // 4, (c // 2) % 2, c % 2)
        pairs.append((c, (z % NZ) * 4 + (hi % 2) * 2 + core % 2))
    return pairs


def along_z(v):
    return lax.ppermute(v, "col", col_pairs(lambda z, hi, core: (z + 1 - 2 * core, hi, core)))


def across_x(v):
    return lax.ppermute(v, "col", col_pairs(lambda z, hi, core: (z, hi + 1, core)))


def other_core(v):
    return lax.ppermute(v, "col", col_pairs(lambda z, hi, core: (z, hi, core + 1)))


def along_y(v):
    pairs = []
    for r in range(8):
        for c in range(32):
            y = (r // 2 + 1 - 2 * (c % 2)) % NY
            pairs.append((r * 32 + c, (y * 2 + r % 2) * 32 + c))
    return lax.ppermute(v, ("row", "col"), pairs)


def beside_x(v):
    return lax.ppermute(v, "row", [(r, r ^ 1) for r in range(8)])


def mask_kernel(mask, values, *outs):
    for i in range(8):
        for j in range(2):
            at = (slice(i * BLOCK, (i + 1) * BLOCK), slice(j * BLOCK, (j + 1) * BLOCK))
            if len(outs) == 1:
                outs[0][at] = values[at] * mask[j, i].astype(jnp.bfloat16)
            else:
                for d, out in enumerate(outs):
                    out[at] = values[(d, *at)] * mask[d, j, i].astype(jnp.bfloat16)


def masked(values, mask):
    n = 1 if len(values.shape) == 2 else values.shape[0]
    vmem = pl.BlockSpec(memory_space=pltpu.VMEM)
    return pl.pallas_call(
        mask_kernel,
        out_shape=[jax.ShapeDtypeStruct(values.shape[-2:], values.dtype)] * n,
        in_specs=[pl.BlockSpec(memory_space=pltpu.SMEM), vmem],
        out_specs=[vmem] * n,
        cost_estimate=pl.CostEstimate(flops=10**6, bytes_accessed=2**20, transcendentals=0),
    )(jnp.swapaxes(mask, -1, -2), values)


def matmul_kernel(parts, n_a, n_b, place, keep, *refs):
    a_refs, refs = refs[:n_a], refs[n_a:]
    b_refs, refs = refs[:n_b], refs[n_b:]
    out, a_vm, b_vm, acc, a_sem, b_sem = refs
    row, col = place[0], place[1]
    y, lo = row // 2, row % 2
    z, hi, core = col // 4, (col // 2) % 2, col % 2
    way = 1 - 2 * core
    n_units = len(parts)

    def start(u):
        delta, far = u // 2, u % 2
        head = 1 - core if 1 <= delta <= 3 else core
        for j, (which, index) in enumerate(parts[u]):
            ref = a_refs[which] if index is None else a_refs[which].at[index]
            pltpu.make_async_copy(ref, a_vm.at[u, (head + j) % 2], a_sem.at[u]).start()
        owner = (z + delta * way + NZ) % NZ
        hops = ((y - owner // 2) * way + NY) % NY
        side = (owner % 2 + lo) % 2
        rows = pl.ds(pl.multiple_of(((hi + far) % 2) * UNIT, UNIT), UNIT)
        for n in range(n_b // 2):

            @pl.when(jnp.logical_and(hops == n // 2, side == n % 2))
            def _():
                for d in range(2):
                    source = b_refs[2 * n + d].at[rows, :]
                    pltpu.make_async_copy(source, b_vm.at[u, d], b_sem.at[u]).start()

    for u in range(AHEAD):
        start(u)
    for u in range(n_units):
        if u + AHEAD < n_units:
            start(u + AHEAD)
        pltpu.make_async_copy(b_vm.at[u], b_vm.at[u], b_sem.at[u]).wait()
        pltpu.make_async_copy(a_vm.at[u], a_vm.at[u], a_sem.at[u]).wait()
        for d in range(2):
            part = sum(
                jnp.dot(
                    a_vm[u, c],
                    b_vm[u, d, c * COLS : (c + 1) * COLS, :],
                    preferred_element_type=jnp.float32,
                )
                for c in range(2)
            )
            if u == 0:
                acc[d] = part
            elif u < n_units - 1:
                acc[d] += part
            else:
                total = acc[d] + part
                for i in range(8):
                    for j in range(2):
                        scale = keep[j, i].astype(jnp.float32)
                        at = (slice(i * BLOCK, (i + 1) * BLOCK), slice(j * BLOCK, (j + 1) * BLOCK))
                        out[(d, *at)] = (total[at] * scale).astype(jnp.bfloat16)


def listed(arrays, array):
    for n, other in enumerate(arrays):
        if other is array:
            return n
    arrays.append(array)
    return len(arrays) - 1


def multiply(place, keep, units, b_arrays):
    a_arrays = []
    parts = [[(listed(a_arrays, v), index) for v, index in unit] for unit in units]
    anywhere = pl.BlockSpec(memory_space=pl.ANY)
    scalars = pl.BlockSpec(memory_space=pltpu.SMEM)
    n_a, n_b = len(a_arrays), len(b_arrays)
    return pl.pallas_call(
        functools.partial(matmul_kernel, parts, n_a, n_b),
        out_shape=jax.ShapeDtypeStruct((2, ROWS, COLS), jnp.bfloat16),
        in_specs=[scalars, scalars] + [anywhere] * (n_a + n_b),
        out_specs=pl.BlockSpec(memory_space=pltpu.VMEM),
        scratch_shapes=[
            pltpu.VMEM((16, 2, ROWS, COLS), jnp.bfloat16),
            pltpu.VMEM((16, 2, UNIT, COLS), jnp.bfloat16),
            pltpu.VMEM((2, ROWS, COLS), jnp.float32),
            pltpu.SemaphoreType.DMA((16,)),
            pltpu.SemaphoreType.DMA((16,)),
        ],
        compiler_params=pltpu.CompilerParams(vmem_limit_bytes=VMEM_LIMIT),
        cost_estimate=pl.CostEstimate(
            flops=2 * 2 * ROWS * COLS * 8 * ROWS, bytes_accessed=25 * 2**20, transcendentals=0
        ),
    )(place, keep, *a_arrays, *b_arrays)


def work(density, density_mask, response, response_mask, filter_mask):
    place = jnp.stack([lax.axis_index("row"), lax.axis_index("col")]).astype(jnp.int32)
    (own,) = masked(density, density_mask)
    b0a, b0b = masked(response, response_mask)

    p0o, across = other_core(own), across_x(own)
    q0 = jnp.stack([across, other_core(across)])
    p1a, p1b = along_z(own), along_z(p0o)
    p2a, p2b = along_z(p1a), along_z(p1b)
    p3a, p3b = along_z(p2a), along_z(p2b)
    p1ao, p1bo = other_core(p1a), other_core(p1b)
    p2ao, p2bo = other_core(p2a), other_core(p2b)
    p3ao, p3bo = other_core(p3a), other_core(p3b)
    p4 = along_z(p3a)
    p4o = other_core(p4)
    q3a, q3b = across_x(p3a), across_x(p3b)
    q3ao, q3bo = other_core(q3a), other_core(q3b)
    q1 = along_z(q0)
    q2 = along_z(q1)
    q1o, q2o = other_core(q1), other_core(q2)
    q4 = along_z(q3a)
    q4o = other_core(q4)

    r1a, r1b = along_y(b0a), along_y(b0b)
    r2a, r2b = along_y(r1a), along_y(r1b)
    r3a, r3b = along_y(r2a), along_y(r2b)
    s0a, s0b = beside_x(b0a), beside_x(b0b)
    s1a, s1b = along_y(s0a), along_y(s0b)
    s2a, s2b = along_y(s1a), beside_x(r2b)
    s3a, s3b = along_y(s2a), along_y(s2b)

    both = lambda v: [(v, 0), (v, 1)]
    two = lambda v, w: [(v, None), (w, None)]
    units = [
        two(own, p0o), both(q0),
        two(p1ao, p1bo), both(q1o),
        two(p2ao, p2bo), both(q2o),
        two(p3ao, p3bo), two(q3ao, q3bo),
        two(p4, p4o), two(q4, q4o),
        two(p3a, p3b), two(q3a, q3b),
        two(p2a, p2b), both(q2),
        two(p1a, p1b), both(q1),
    ]
    b_arrays = [b0a, b0b, s0a, s0b, r1a, r1b, s1a, s1b, r2a, r2b, s2a, s2b, r3a, r3b, s3a, s3b]
    return multiply(place, jnp.swapaxes(filter_mask, 0, 1), units, b_arrays)


def solution(mesh):
    in_specs = (
        P("row", "col"),
        P("row", "col"),
        P(None, "row", "col"),
        P(None, "row", "col"),
        P("row", "col"),
    )
    out_specs = P(None, "row", "col")
    return jax.shard_map(work, mesh=mesh, in_specs=in_specs, out_specs=out_specs, check_vma=False)
```

```python
import functools

import jax
import jax.numpy as jnp
from jax import lax
from jax.experimental import pallas as pl
from jax.experimental.pallas import tpu as pltpu
from jax.sharding import PartitionSpec as P


BLOCK = 128
ROWS = 1024
COLS = 256
UNIT = 512
VMEM_LIMIT = 60 * 2**20
AHEAD = 3
EARLY = [0, 2, 14, 4, 12, 6, 10]
LATE = [1, 3, 15, 5, 13, 7, 11, 9, 8]
NZ, NY = 8, 4


def col_pairs(step):
    pairs = []
    for c in range(32):
        z, hi, core = step(c // 4, (c // 2) % 2, c % 2)
        pairs.append((c, (z % NZ) * 4 + (hi % 2) * 2 + core % 2))
    return pairs


def along_z(v):
    return lax.ppermute(v, "col", col_pairs(lambda z, hi, core: (z + 1 - 2 * core, hi, core)))


def across_x(v):
    return lax.ppermute(v, "col", col_pairs(lambda z, hi, core: (z, hi + 1, core)))


def other_core(v):
    return lax.ppermute(v, "col", col_pairs(lambda z, hi, core: (z, hi, core + 1)))


def along_y(v):
    pairs = []
    for r in range(8):
        for c in range(32):
            y = (r // 2 + 1 - 2 * (c % 2)) % NY
            pairs.append((r * 32 + c, (y * 2 + r % 2) * 32 + c))
    return lax.ppermute(v, ("row", "col"), pairs)


def beside_x(v):
    return lax.ppermute(v, "row", [(r, r ^ 1) for r in range(8)])


def mask_kernel(mask, values, *outs):
    for d, out in enumerate(outs):
        for i in range(8):
            for j in range(2):
                at = (slice(i * BLOCK, (i + 1) * BLOCK), slice(j * BLOCK, (j + 1) * BLOCK))
                out[at] = values[(d, *at)] * mask[d, j, i].astype(jnp.bfloat16)


def masked_pair(values, mask):
    vmem = pl.BlockSpec(memory_space=pltpu.VMEM)
    return pl.pallas_call(
        mask_kernel,
        out_shape=[jax.ShapeDtypeStruct(values.shape[1:], values.dtype)] * 2,
        in_specs=[pl.BlockSpec(memory_space=pltpu.SMEM), vmem],
        out_specs=[vmem] * 2,
        cost_estimate=pl.CostEstimate(flops=10**6, bytes_accessed=2**22, transcendentals=0),
    )(jnp.swapaxes(mask, 1, 2), values)


def masked(values, mask):
    shaped = values.reshape(ROWS // BLOCK, BLOCK, COLS // BLOCK, BLOCK)
    scaled = shaped * mask.astype(values.dtype)[:, None, :, None]
    return scaled.reshape(values.shape)


def whereabouts():
    row, col = lax.axis_index("row"), lax.axis_index("col")
    y, lo = row // 2, row % 2
    z, hi, core = col // 4, (col // 2) % 2, col % 2
    return y, lo, z, hi, core, 1 - 2 * core


class Fetch:
    def __init__(self, parts, a_refs, b_refs, a_vm, b_vm, a_sem, b_sem):
        self.y, self.lo, self.z, self.hi, self.core, self.way = whereabouts()
        self.parts, self.a_refs, self.b_refs = parts, a_refs, b_refs
        self.a_vm, self.b_vm, self.a_sem, self.b_sem = a_vm, b_vm, a_sem, b_sem

    def origin(self, u):
        owner = (self.z + (u // 2) * self.way + NZ) % NZ
        hops = ((self.y - owner // 2) * self.way + NY) % NY
        return hops, (owner % 2 + self.lo) % 2

    def start_a(self, u, slot):
        head = 1 - self.core if 1 <= u // 2 <= 3 else self.core
        for j, (which, index) in enumerate(self.parts[u]):
            ref = self.a_refs[which] if index is None else self.a_refs[which].at[index]
            to = self.a_vm.at[slot, (head + j) % 2]
            pltpu.make_async_copy(ref, to, self.a_sem.at[slot]).start()

    def start_b(self, far, hops, side, slot, choices):
        rows = pl.ds(pl.multiple_of(((self.hi + far) % 2) * UNIT, UNIT), UNIT)
        for n in choices:

            @pl.when(jnp.logical_and(hops == n // 2, side == n % 2))
            def _():
                for d in range(2):
                    source = self.b_refs[2 * n + d].at[rows, :]
                    to = self.b_vm.at[slot, d]
                    pltpu.make_async_copy(source, to, self.b_sem.at[slot]).start()

    def start(self, u, slot):
        self.start_a(u, slot)
        self.start_b(u % 2, *self.origin(u), slot, range(len(self.b_refs) // 2))

    def wait(self, slot):
        for vm, sem in ((self.b_vm, self.b_sem), (self.a_vm, self.a_sem)):
            pltpu.make_async_copy(vm.at[slot], vm.at[slot], sem.at[slot]).wait()

    def product(self, slot, d):
        return sum(
            jnp.dot(
                self.a_vm[slot, c],
                self.b_vm[slot, d, c * COLS : (c + 1) * COLS, :],
                preferred_element_type=jnp.float32,
            )
            for c in range(2)
        )


def early_kernel(parts, n_a, n_b, *refs):
    out, a_vm, b_vm, acc, a_sem, b_sem, acc_sem = refs[n_a + n_b :]
    fetch = Fetch(parts, refs[:n_a], refs[n_a : n_a + n_b], a_vm, b_vm, a_sem, b_sem)

    def due(n):
        return fetch.origin(EARLY[n])[0] != 3

    def start(n):
        pl.when(due(n))(lambda: fetch.start(EARLY[n], n))

    def add(n):
        fetch.wait(n)
        for d in range(2):
            acc[d] += fetch.product(n, d)

    for n in range(AHEAD + 1):
        start(n)
    acc[...] = jnp.zeros_like(acc)
    for n in range(len(EARLY)):
        if n + AHEAD + 1 < len(EARLY):
            start(n + AHEAD + 1)
        pl.when(due(n))(functools.partial(add, n))
    store = pltpu.make_async_copy(acc, out, acc_sem)
    store.start()
    store.wait()


def late_kernel(parts, n_a, n_b, *refs):
    before, keep_in, out, a_vm, b_vm, acc, earlier, *refs_left = refs[n_a + n_b :]
    a_sem, b_sem, acc_sem, keep, done, out_sem = refs_left
    fetch = Fetch(parts, refs[:n_a], refs[n_a : n_a + n_b], a_vm, b_vm, a_sem, b_sem)
    n_late = len(LATE)

    owner_y = (fetch.y - 3 * fetch.way + 3 * NY) % NY
    deltas = [((owner_y * 2 + t - fetch.z) * fetch.way + 2 * NZ) % NZ for t in range(2)]

    def start(n):
        if n < n_late:
            fetch.start(LATE[n], n)
            return
        t = n - n_late
        for u in EARLY:
            pl.when(deltas[t] == u // 2)(functools.partial(fetch.start_a, u, n))

        @pl.when(deltas[t] != 4)
        def _():
            fetch.start_b(0, 3, (t + fetch.lo) % 2, n, (6, 7))

    def add(n):
        fetch.wait(n)
        for d in range(2):
            acc[d] += fetch.product(n, d)

    order = [*range(n_late - 1), n_late, n_late + 1, n_late - 1]
    for n in order[:AHEAD]:
        start(n)
    load = pltpu.make_async_copy(before, earlier, acc_sem.at[0])
    keep_load = pltpu.make_async_copy(keep_in, keep, acc_sem.at[1])
    stores = [pltpu.make_async_copy(done.at[d], out.at[d], out_sem.at[d]) for d in range(2)]
    for i, n in enumerate(order):
        if i + AHEAD < len(order):
            start(order[i + AHEAD])
        if i == 0:
            load.start()
            keep_load.start()
            fetch.wait(n)
            for d in range(2):
                acc[d] = fetch.product(n, d)
        elif i < len(order) - 1:
            if n < n_late:
                add(n)
            else:
                pl.when(deltas[n - n_late] != 4)(functools.partial(add, n))
        else:
            fetch.wait(n)
            load.wait()
            keep_load.wait()
            for d in range(2):
                total = acc[d] + earlier[d] + fetch.product(n, d)
                for i in range(8):
                    for j in range(2):
                        scale = keep[j, i].astype(jnp.float32)
                        at = (slice(i * BLOCK, (i + 1) * BLOCK), slice(j * BLOCK, (j + 1) * BLOCK))
                        done[(d, *at)] = (total[at] * scale).astype(jnp.bfloat16)
                stores[d].start()
    for store in stores:
        store.wait()


def listed(arrays, array):
    for n, other in enumerate(arrays):
        if other is array:
            return n
    arrays.append(array)
    return len(arrays) - 1


def multiply(units, b_arrays, before=None, keep=None):
    late = before is not None
    a_arrays, parts = [], {}
    for u, unit in enumerate(units):
        if late or u in EARLY:
            parts[u] = [(listed(a_arrays, v), index) for v, index in unit]
    operands = [*a_arrays, *b_arrays] + ([before, keep] if late else [])
    slots = len(LATE) + 2 if late else len(EARLY)
    total = pltpu.VMEM((2, ROWS, COLS), jnp.float32)
    scratch = [
        pltpu.VMEM((slots, 2, ROWS, COLS), jnp.bfloat16),
        pltpu.VMEM((slots, 2, UNIT, COLS), jnp.bfloat16),
        *[total] * (1 + late),
        pltpu.SemaphoreType.DMA((slots,)),
        pltpu.SemaphoreType.DMA((slots,)),
    ]
    if late:
        scratch += [
            pltpu.SemaphoreType.DMA((2,)),
            pltpu.SMEM(keep.shape, keep.dtype),
            pltpu.VMEM((2, ROWS, COLS), jnp.bfloat16),
            pltpu.SemaphoreType.DMA((2,)),
        ]
    else:
        scratch.append(pltpu.SemaphoreType.DMA)
    kernel = late_kernel if late else early_kernel
    return pl.pallas_call(
        functools.partial(kernel, parts, len(a_arrays), len(b_arrays)),
        out_shape=jax.ShapeDtypeStruct((2, ROWS, COLS), jnp.bfloat16 if late else jnp.float32),
        in_specs=[pl.BlockSpec(memory_space=pl.ANY)] * len(operands),
        out_specs=pl.BlockSpec(memory_space=pl.ANY),
        scratch_shapes=scratch,
        compiler_params=pltpu.CompilerParams(vmem_limit_bytes=VMEM_LIMIT),
        cost_estimate=pl.CostEstimate(
            flops=2 * 2 * ROWS * COLS * UNIT * slots,
            bytes_accessed=slots * 3 * 2**19,
            transcendentals=0,
        ),
    )(*operands)


def work(density, density_mask, response, response_mask, filter_mask):
    own = masked(density, density_mask)
    b0a, b0b = masked_pair(response, response_mask)

    p0o, across = other_core(own), across_x(own)
    q0 = jnp.stack([across, other_core(across)])
    p1a, p1b = along_z(own), along_z(p0o)
    p2a, p2b = along_z(p1a), along_z(p1b)
    p3a, p3b = along_z(p2a), along_z(p2b)
    p1ao, p1bo = other_core(p1a), other_core(p1b)
    p2ao, p2bo = other_core(p2a), other_core(p2b)
    p3ao, p3bo = other_core(p3a), other_core(p3b)
    p4 = along_z(p3a)
    p4o = other_core(p4)
    q3a, q3b = across_x(p3a), across_x(p3b)
    q3ao, q3bo = other_core(q3a), other_core(q3b)
    q1 = along_z(q0)
    q2 = along_z(q1)
    q1o, q2o = other_core(q1), other_core(q2)
    q4 = along_z(q3a)
    q4o = other_core(q4)

    r1a, r1b = along_y(b0a), along_y(b0b)
    r2a, r2b = along_y(r1a), along_y(r1b)
    r3a, r3b = along_y(r2a), along_y(r2b)
    s0a, s0b = beside_x(b0a), beside_x(b0b)
    s1a, s1b = along_y(s0a), along_y(s0b)
    s2a, s2b = along_y(s1a), beside_x(r2b)
    s3a, s3b = along_y(s2a), along_y(s2b)

    both = lambda v: [(v, 0), (v, 1)]
    two = lambda v, w: [(v, None), (w, None)]
    units = [
        two(own, p0o), both(q0),
        two(p1ao, p1bo), both(q1o),
        two(p2ao, p2bo), both(q2o),
        two(p3ao, p3bo), two(q3ao, q3bo),
        two(p4, p4o), two(q4, q4o),
        two(p3a, p3b), two(q3a, q3b),
        two(p2a, p2b), both(q2),
        two(p1a, p1b), both(q1),
    ]
    b_arrays = [b0a, b0b, s0a, s0b, r1a, r1b, s1a, s1b, r2a, r2b, s2a, s2b]
    keep = jnp.swapaxes(filter_mask, 0, 1)
    total = multiply(units, b_arrays)
    return multiply(units, b_arrays + [r3a, r3b, s3a, s3b], total, keep)


def solution(mesh):
    in_specs = (
        P("row", "col"),
        P("row", "col"),
        P(None, "row", "col"),
        P(None, "row", "col"),
        P("row", "col"),
    )
    out_specs = P(None, "row", "col")
    return jax.shard_map(work, mesh=mesh, in_specs=in_specs, out_specs=out_specs, check_vma=False)
```

```python
import functools

import jax
import jax.numpy as jnp
from jax import lax
from jax.experimental import pallas as pl
from jax.experimental.pallas import tpu as pltpu
from jax.sharding import PartitionSpec as P


BLOCK = 128
ROWS = 1024
COLS = 256
UNIT = 512
AHEAD = 3
EARLY = [0, 2, 14, 4, 12, 6, 10]
LATE = [1, 3, 15, 5, 13, 7, 11, 9, 8]
NZ, NY = 8, 4


def col_pairs(step):
    pairs = []
    for c in range(32):
        z, hi, core = step(c // 4, (c // 2) % 2, c % 2)
        pairs.append((c, (z % NZ) * 4 + (hi % 2) * 2 + core % 2))
    return pairs


def along_z(v):
    return lax.ppermute(v, "col", col_pairs(lambda z, hi, core: (z + 1 - 2 * core, hi, core)))


def across_x(v):
    return lax.ppermute(v, "col", col_pairs(lambda z, hi, core: (z, hi + 1, core)))


def other_core(v):
    return lax.ppermute(v, "col", col_pairs(lambda z, hi, core: (z, hi, core + 1)))


def along_y(v):
    pairs = []
    for r in range(8):
        for c in range(32):
            y = (r // 2 + 1 - 2 * (c % 2)) % NY
            pairs.append((r * 32 + c, (y * 2 + r % 2) * 32 + c))
    return lax.ppermute(v, ("row", "col"), pairs)


def beside_x(v):
    return lax.ppermute(v, "row", [(r, r ^ 1) for r in range(8)])


def mask_kernel(mask, values, *outs):
    for d, out in enumerate(outs):
        for i in range(8):
            for j in range(2):
                at = (slice(i * BLOCK, (i + 1) * BLOCK), slice(j * BLOCK, (j + 1) * BLOCK))
                out[at] = values[(d, *at)] * mask[d, j, i].astype(jnp.bfloat16)


def masked_pair(values, mask):
    vmem = pl.BlockSpec(memory_space=pltpu.VMEM)
    return pl.pallas_call(
        mask_kernel,
        out_shape=[jax.ShapeDtypeStruct(values.shape[1:], values.dtype)] * 2,
        in_specs=[pl.BlockSpec(memory_space=pltpu.SMEM), vmem],
        out_specs=[vmem] * 2,
        cost_estimate=pl.CostEstimate(flops=10**6, bytes_accessed=2**22, transcendentals=0),
    )(jnp.swapaxes(mask, 1, 2), values)


def masked(values, mask):
    shaped = values.reshape(ROWS // BLOCK, BLOCK, COLS // BLOCK, BLOCK)
    scaled = shaped * mask.astype(values.dtype)[:, None, :, None]
    return scaled.reshape(values.shape)


def whereabouts():
    row, col = lax.axis_index("row"), lax.axis_index("col")
    y, lo = row // 2, row % 2
    z, hi, core = col // 4, (col // 2) % 2, col % 2
    return y, lo, z, hi, core, 1 - 2 * core


class Fetch:
    def __init__(self, parts, a_refs, b_refs, a_vm, b_vm, a_sem, b_sem):
        self.y, self.lo, self.z, self.hi, self.core, self.way = whereabouts()
        self.parts, self.a_refs, self.b_refs = parts, a_refs, b_refs
        self.a_vm, self.b_vm, self.a_sem, self.b_sem = a_vm, b_vm, a_sem, b_sem

    def origin(self, u):
        owner = (self.z + (u // 2) * self.way + NZ) % NZ
        hops = ((self.y - owner // 2) * self.way + NY) % NY
        return hops, (owner % 2 + self.lo) % 2

    def start_a(self, u, slot):
        head = 1 - self.core if 1 <= u // 2 <= 3 else self.core
        for j, (which, index) in enumerate(self.parts[u]):
            ref = self.a_refs[which] if index is None else self.a_refs[which].at[index]
            to = self.a_vm.at[slot, (head + j) % 2]
            pltpu.make_async_copy(ref, to, self.a_sem.at[slot]).start()

    def start_b(self, far, hops, side, slot, choices):
        rows = pl.ds(pl.multiple_of(((self.hi + far) % 2) * UNIT, UNIT), UNIT)
        for n in choices:

            @pl.when(jnp.logical_and(hops == n // 2, side == n % 2))
            def _():
                for d in range(2):
                    source = self.b_refs[2 * n + d].at[rows, :]
                    to = self.b_vm.at[slot, d]
                    pltpu.make_async_copy(source, to, self.b_sem.at[slot]).start()

    def start(self, u, slot):
        self.start_a(u, slot)
        self.start_b(u % 2, *self.origin(u), slot, range(len(self.b_refs) // 2))

    def wait(self, slot):
        for vm, sem in ((self.b_vm, self.b_sem), (self.a_vm, self.a_sem)):
            pltpu.make_async_copy(vm.at[slot], vm.at[slot], sem.at[slot]).wait()

    def product(self, slot, d):
        return sum(
            jnp.dot(
                self.a_vm[slot, c],
                self.b_vm[slot, d, c * COLS : (c + 1) * COLS, :],
                preferred_element_type=jnp.float32,
            )
            for c in range(2)
        )


def early_kernel(parts, n_a, n_b, *refs):
    out, a_vm, b_vm, acc, a_sem, b_sem, acc_sem = refs[n_a + n_b :]
    fetch = Fetch(parts, refs[:n_a], refs[n_a : n_a + n_b], a_vm, b_vm, a_sem, b_sem)

    def due(n):
        return fetch.origin(EARLY[n])[0] != 3

    def start(n):
        pl.when(due(n))(lambda: fetch.start(EARLY[n], n))

    def add(n):
        fetch.wait(n)
        for d in range(2):
            acc[d] += fetch.product(n, d)

    for n in range(AHEAD + 1):
        start(n)
    acc[...] = jnp.zeros_like(acc)
    for n in range(len(EARLY)):
        if n + AHEAD + 1 < len(EARLY):
            start(n + AHEAD + 1)
        pl.when(due(n))(functools.partial(add, n))
    store = pltpu.make_async_copy(acc, out, acc_sem)
    store.start()
    store.wait()


def late_kernel(parts, n_a, n_b, *refs):
    before, keep_in, out, a_vm, b_vm, acc, earlier, *refs_left = refs[n_a + n_b :]
    a_sem, b_sem, acc_sem, keep, done, out_sem = refs_left
    fetch = Fetch(parts, refs[:n_a], refs[n_a : n_a + n_b], a_vm, b_vm, a_sem, b_sem)
    n_late = len(LATE)

    owner_y = (fetch.y - 3 * fetch.way + 3 * NY) % NY
    deltas = [((owner_y * 2 + t - fetch.z) * fetch.way + 2 * NZ) % NZ for t in range(2)]

    def start(n):
        if n < n_late:
            fetch.start(LATE[n], n)
            return
        t = n - n_late
        for u in EARLY:
            pl.when(deltas[t] == u // 2)(functools.partial(fetch.start_a, u, n))

        @pl.when(deltas[t] != 4)
        def _():
            fetch.start_b(0, 3, (t + fetch.lo) % 2, n, (6, 7))

    def add(n):
        fetch.wait(n)
        for d in range(2):
            acc[d] += fetch.product(n, d)

    order = [*range(n_late - 1), n_late, n_late + 1, n_late - 1]
    for n in order[:AHEAD]:
        start(n)
    load = pltpu.make_async_copy(before, earlier, acc_sem.at[0])
    keep_load = pltpu.make_async_copy(keep_in, keep, acc_sem.at[1])
    stores = [pltpu.make_async_copy(done.at[d], out.at[d], out_sem.at[d]) for d in range(2)]
    for i, n in enumerate(order):
        if i + AHEAD < len(order):
            start(order[i + AHEAD])
        if i == 0:
            load.start()
            keep_load.start()
            fetch.wait(n)
            for d in range(2):
                acc[d] = fetch.product(n, d)
        elif i < len(order) - 1:
            if n < n_late:
                add(n)
            else:
                pl.when(deltas[n - n_late] != 4)(functools.partial(add, n))
        else:
            fetch.wait(n)
            load.wait()
            keep_load.wait()
            for d in range(2):
                total = acc[d] + earlier[d] + fetch.product(n, d)
                for i in range(8):
                    for j in range(2):
                        scale = keep[j, i].astype(jnp.float32)
                        at = (slice(i * BLOCK, (i + 1) * BLOCK), slice(j * BLOCK, (j + 1) * BLOCK))
                        done[(d, *at)] = (total[at] * scale).astype(jnp.bfloat16)
                stores[d].start()
    for store in stores:
        store.wait()


def listed(arrays, array):
    for n, other in enumerate(arrays):
        if other is array:
            return n
    arrays.append(array)
    return len(arrays) - 1


def multiply(units, b_arrays, before=None, keep=None):
    late = before is not None
    a_arrays, parts = [], {}
    for u, unit in enumerate(units):
        if late or u in EARLY:
            parts[u] = [(listed(a_arrays, v), index) for v, index in unit]
    n_pieces = len(a_arrays) + len(b_arrays)
    operands = [*a_arrays, *b_arrays] + ([before, keep] if late else [])
    slots = len(LATE) + 2 if late else len(EARLY)
    total = pltpu.VMEM((2, ROWS, COLS), jnp.float32)
    scratch = [
        pltpu.VMEM((slots, 2, ROWS, COLS), jnp.bfloat16),
        pltpu.VMEM((slots, 2, UNIT, COLS), jnp.bfloat16),
        *[total] * (1 + late),
        pltpu.SemaphoreType.DMA((slots,)),
        pltpu.SemaphoreType.DMA((slots,)),
    ]
    if late:
        scratch += [
            pltpu.SemaphoreType.DMA((2,)),
            pltpu.SMEM(keep.shape, keep.dtype),
            pltpu.VMEM((2, ROWS, COLS), jnp.bfloat16),
            pltpu.SemaphoreType.DMA((2,)),
        ]
    else:
        scratch.append(pltpu.SemaphoreType.DMA)
    kernel = late_kernel if late else early_kernel
    return pl.pallas_call(
        functools.partial(kernel, parts, len(a_arrays), len(b_arrays)),
        out_shape=jax.ShapeDtypeStruct((2, ROWS, COLS), jnp.bfloat16 if late else jnp.float32),
        in_specs=[pl.BlockSpec(memory_space=pltpu.HBM)] * n_pieces
        + [pl.BlockSpec(memory_space=pl.ANY)] * (len(operands) - n_pieces),
        out_specs=pl.BlockSpec(memory_space=pl.ANY),
        scratch_shapes=scratch,
        compiler_params=pltpu.CompilerParams(vmem_limit_bytes=30 * 2**20),
        cost_estimate=pl.CostEstimate(
            flops=2 * 2 * ROWS * COLS * UNIT * slots,
            bytes_accessed=slots * 3 * 2**19,
            transcendentals=0,
        ),
    )(*operands)


def work(density, density_mask, response, response_mask, filter_mask):
    own = masked(density, density_mask)
    b0a, b0b = masked_pair(response, response_mask)

    p0o, across = other_core(own), across_x(own)
    q0 = jnp.stack([across, other_core(across)])
    p1a, p1b = along_z(own), along_z(p0o)
    p2a, p2b = along_z(p1a), along_z(p1b)
    p3a, p3b = along_z(p2a), along_z(p2b)
    p1ao, p1bo = other_core(p1a), other_core(p1b)
    p2ao, p2bo = other_core(p2a), other_core(p2b)
    p3ao, p3bo = other_core(p3a), other_core(p3b)
    p4 = along_z(p3a)
    p4o = other_core(p4)
    q3a, q3b = across_x(p3a), across_x(p3b)
    q3ao, q3bo = other_core(q3a), other_core(q3b)
    q1 = along_z(q0)
    q2 = along_z(q1)
    q1o, q2o = other_core(q1), other_core(q2)
    q4 = along_z(q3a)
    q4o = other_core(q4)

    r1a, r1b = along_y(b0a), along_y(b0b)
    r2a, r2b = along_y(r1a), along_y(r1b)
    r3a, r3b = along_y(r2a), along_y(r2b)
    s0a, s0b = beside_x(b0a), beside_x(b0b)
    s1a, s1b = along_y(s0a), along_y(s0b)
    s2a, s2b = along_y(s1a), beside_x(r2b)
    s3a, s3b = along_y(s2a), along_y(s2b)

    both = lambda v: [(v, 0), (v, 1)]
    two = lambda v, w: [(v, None), (w, None)]
    units = [
        two(own, p0o), both(q0),
        two(p1ao, p1bo), both(q1o),
        two(p2ao, p2bo), both(q2o),
        two(p3ao, p3bo), two(q3ao, q3bo),
        two(p4, p4o), two(q4, q4o),
        two(p3a, p3b), two(q3a, q3b),
        two(p2a, p2b), both(q2),
        two(p1a, p1b), both(q1),
    ]
    b_arrays = [b0a, b0b, s0a, s0b, r1a, r1b, s1a, s1b, r2a, r2b, s2a, s2b]
    keep = jnp.swapaxes(filter_mask, 0, 1)
    total = multiply(units, b_arrays)
    return multiply(units, b_arrays + [r3a, r3b, s3a, s3b], total, keep)


def solution(mesh):
    in_specs = (
        P("row", "col"),
        P("row", "col"),
        P(None, "row", "col"),
        P(None, "row", "col"),
        P("row", "col"),
    )
    out_specs = P(None, "row", "col")
    return jax.shard_map(work, mesh=mesh, in_specs=in_specs, out_specs=out_specs, check_vma=False)
```
